32 devices in a mesh: bank: 4 (over x, core), zero: 8 (over z, y).
Axes of the slice: x: 2, y: 2, z: 4, core: 2. Of those that a mesh axis runs over, the one named last changes fastest.
Arguments:
- train_gate: float32 [128, 2048, 768], P('bank', 'zero'), may hold values from -0.1875 to 0.1875
- other_gate: bfloat16 [128, 2048, 768], P('bank', 'zero'), may hold values from -0.0625 to 0.0625
- train_up: float32 [128, 2048, 768], P('bank', 'zero'), may hold values from -0.1875 to 0.1875
- other_up: bfloat16 [128, 2048, 768], P('bank', 'zero'), may hold values from -0.0625 to 0.0625
- router_weight: float32 [2048, 128], P('zero', 'bank'), may hold values from -0.125 to 0.125
- router_gain: float32 [2048], P('zero'), may hold values from 0.25 to 1.75
Outputs:
- ready_gate: bfloat16 [128, 2048, 768], P('bank', None, 'zero')
- ready_up: bfloat16 [128, 2048, 768], P('bank', None, 'zero')
- scale_gate: float32 [128, 768], P('bank', 'zero')
- scale_up: float32 [128, 768], P('bank', 'zero')
- serve_router: bfloat16 [2048, 128], replicated
The draws below stay inside these ranges and needn't reach their ends.
All inputs are finite; a program needn't handle non-finite values. Where the reference program divides by a largest or mean magnitude, that divisor is 1e-20 or more.
Results may differ from the reference program's by a relative error of at most 0.001.
Values may be sent and summed in bfloat16 or wider, within the bound.
No kernel may reach another device: no remote copies, remote signals or barrier semaphores. Data moves between devices by JAX's collectives and lax.ppermute only.
A program may use at most 256 MiB of HBM per device.

```python
import jax
import jax.numpy as jnp

EXPERTS = 128
D_MODEL = 2048
D_EXPERT = 768


def raised(array, rng, source, target, parts, factor):
    owner, partner = [(jnp.arange(array.shape[axis_at]) // (array.shape[axis_at] // parts)).reshape([-1 if axis == axis_at else 1 for axis in range(array.ndim)]) for axis_at in (source, target)]
    chosen = jax.random.permutation(rng, parts)[partner]
    strong = (owner == chosen) | (owner == (partner + parts // 2) % parts)
    return jnp.where(strong, factor * array, array)


def level_of(rng, extent, pieces, smallest, high):
    factor_of, own = 1.0, jax.random.fold_in(rng, 6)
    for position, blocks in pieces:
        draws = jnp.exp(jax.random.uniform(jax.random.fold_in(own, position), (blocks,), jnp.float32, smallest / len(pieces), high / len(pieces)))
        factor_of = factor_of * jnp.repeat(draws, extent[position] // blocks).reshape([-1 if axis == position else 1 for axis in range(len(extent))])
    return factor_of


def scatter_about(own_key, extent, scale, reach, split=(), dtype=jnp.bfloat16):
    loudness = level_of(own_key, extent, split, -0.22, 0.18) if split else 1.0
    entries = jax.random.normal(own_key, extent, jnp.float32) * scale * loudness
    return jnp.minimum(jnp.maximum(entries, -reach), reach).astype(dtype)


def heavy_noise(rng, dims, width, most, pieces, heavy, held_as=jnp.bfloat16):
    array = width * jax.random.normal(rng, dims, jnp.float32)
    if pieces:
        array = array * level_of(rng, dims, pieces, -0.22, 0.18)
    return jnp.clip(raised(array, jax.random.fold_in(rng, 3), *heavy), -most, most).astype(held_as)


def setup_inputs(seed: int = 0) -> dict:
    arg_keys = jax.random.split(jax.random.key(seed), 7)
    return {
        "train_gate": heavy_noise(arg_keys[0], (EXPERTS, D_MODEL, D_EXPERT), D_MODEL ** -0.5, 0.1875, ((0, 4), (1, 8)), (1, 2, 8, 2.0), jnp.float32),
        "other_gate": scatter_about(arg_keys[1], (EXPERTS, D_MODEL, D_EXPERT), (D_MODEL * 4) ** -0.5, 0.0625, ((0, 4), (1, 8))),
        "train_up": heavy_noise(arg_keys[2], (EXPERTS, D_MODEL, D_EXPERT), D_MODEL ** -0.5, 0.1875, ((0, 4), (1, 8)), (1, 2, 8, 2.0), jnp.float32),
        "other_up": scatter_about(arg_keys[3], (EXPERTS, D_MODEL, D_EXPERT), (D_MODEL * 4) ** -0.5, 0.0625, ((0, 4), (1, 8))),
        "router_weight": scatter_about(arg_keys[4], (D_MODEL, EXPERTS), D_MODEL ** -0.5, 0.125, ((0, 8), (1, 4)), jnp.float32),
        "router_gain": jnp.clip(1.0 + 0.15 * jax.random.normal(arg_keys[5], (D_MODEL,), jnp.float32), 0.25, 1.75),
    }


def reference(train_gate, other_gate, train_up, other_up, router_weight, router_gain):
    latest_gate = train_gate + other_gate.astype(jnp.float32)
    latest_up = train_up + other_up.astype(jnp.float32)
    scale_gate = jnp.max(jnp.abs(latest_gate), axis=1)
    ready_gate = (latest_gate / jnp.expand_dims(scale_gate, 1)).astype(jnp.bfloat16)
    scale_up = jnp.max(jnp.abs(latest_up), axis=1)
    ready_up = (latest_up / jnp.expand_dims(scale_up, 1)).astype(jnp.bfloat16)
    serve_router = (router_weight * router_gain[:, None]).astype(jnp.bfloat16)
    return ready_gate, ready_up, scale_gate, scale_up, serve_router
```

```python
import functools

import jax
import jax.numpy as jnp
from jax import lax
from jax.experimental import pallas as pl
from jax.experimental.pallas import tpu as pltpu
from jax.sharding import PartitionSpec as P

VMEM_LIMIT = 48 * 1024 * 1024


def cost(flops, moved):
    return pl.CostEstimate(flops=flops, bytes_accessed=moved, transcendentals=0)


def max_kernel(train_ref, other_ref, out_ref):
    latest = train_ref[...] + other_ref[...].astype(jnp.float32)
    out_ref[...] = jnp.max(jnp.abs(latest), axis=1, keepdims=True)


def column_max(train, other, first, count):
    _, rows, columns = train.shape
    step = 4 if count % 4 == 0 and first % 4 == 0 else 1
    at = lambda i: (first // step + i, 0, 0)
    return pl.pallas_call(
        max_kernel,
        grid=(count // step,),
        in_specs=[pl.BlockSpec((step, rows, columns), at)] * 2,
        out_specs=pl.BlockSpec((step, 1, columns), lambda i: (i, 0, 0)),
        out_shape=jax.ShapeDtypeStruct((count, 1, columns), jnp.float32),
        cost_estimate=cost(count * rows * columns * 60, count * rows * columns * 6),
        compiler_params=pltpu.CompilerParams(vmem_limit_bytes=VMEM_LIMIT),
        name="column_max",
    )(train, other)


def narrow_kernel(parts, train_ref, other_ref, scale_ref, out_ref):
    for e in range(train_ref.shape[0]):
        latest = train_ref[e] + other_ref[e].astype(jnp.float32)
        turned = (latest / scale_ref[e]).T
        width = turned.shape[0] // parts
        for d in range(parts):
            out_ref[d, e] = turned[d * width : (d + 1) * width].astype(jnp.bfloat16)


def narrow(train, other, scale, first, count, parts):
    _, rows, columns = train.shape
    step = 2 if count % 2 == 0 and first % 2 == 0 else 1
    at = lambda i: (first // step + i, 0, 0)
    return pl.pallas_call(
        functools.partial(narrow_kernel, parts),
        grid=(count // step,),
        in_specs=[pl.BlockSpec((step, rows, columns), at)] * 2
        + [pl.BlockSpec((step, 1, columns), lambda i: (i, 0, 0))],
        out_specs=pl.BlockSpec((parts, step, columns // parts, rows), lambda i: (0, i, 0, 0)),
        out_shape=jax.ShapeDtypeStruct((parts, count, columns // parts, rows), jnp.bfloat16),
        cost_estimate=cost(count * rows * columns * 100, count * rows * columns * 8),
        compiler_params=pltpu.CompilerParams(vmem_limit_bytes=VMEM_LIMIT),
        name="narrow",
    )(train, other, scale)


def place_kernel(in_ref, *refs):
    out_ref = refs[-1]
    rows = in_ref.shape[3]
    for s in range(in_ref.shape[0]):
        out_ref[:, :, s * rows : (s + 1) * rows] = in_ref[s]


def place(received, held, first, experts):
    parts, count, width, rows = received.shape
    step = 2 if count % 2 == 0 and first % 2 == 0 else 1
    specs = [pl.BlockSpec((parts, step, width, rows), lambda i: (0, i, 0, 0))]
    args = [received]
    if held is not None:
        specs.append(pl.BlockSpec(memory_space=pl.ANY))
        args.append(held)
    return pl.pallas_call(
        place_kernel,
        grid=(count // step,),
        in_specs=specs,
        out_specs=pl.BlockSpec((step, width, parts * rows), lambda i: (first // step + i, 0, 0)),
        out_shape=jax.ShapeDtypeStruct((experts, width, parts * rows), jnp.bfloat16),
        input_output_aliases={} if held is None else {1: 0},
        cost_estimate=cost(parts * count * width * rows * 40, parts * count * width * rows * 4),
        compiler_params=pltpu.CompilerParams(vmem_limit_bytes=VMEM_LIMIT),
        name="place",
    )(*args)


def route(router_weight, router_gain):
    part = (router_weight * router_gain[:, None]).astype(jnp.bfloat16)
    row = lax.all_gather(part, "zero", axis=0, tiled=True)
    return lax.all_gather(row, "bank", axis=1, tiled=True)


def plain(train_gate, other_gate, train_up, other_up, router_weight, router_gain):
    latest = [t + o.astype(jnp.float32) for t, o in ((train_gate, other_gate), (train_up, other_up))]
    scales = lax.pmax([jnp.max(jnp.abs(a), axis=1) for a in latest], "zero")
    ready, own = [], []
    for a, s in zip(latest, scales):
        thin = (a / s[:, None]).astype(jnp.bfloat16)
        ready.append(lax.all_to_all(thin, "zero", split_axis=2, concat_axis=1, tiled=True))
        width = ready[-1].shape[2]
        own.append(lax.dynamic_slice_in_dim(s, lax.axis_index("zero") * width, width, axis=1))
    return (*ready, *own, route(router_weight, router_gain))


def chunked(parts, train_gate, other_gate, train_up, other_up, router_weight, router_gain):
    pairs = ((train_gate, other_gate), (train_up, other_up))
    experts, rows, columns = train_gate.shape
    half, lead = experts // 2, experts // 4 * 3
    chunks = ((0, 0, lead), (0, lead, experts - lead), (1, 0, half), (1, half, half))
    width = columns // parts

    def exchange(block):
        return lax.all_to_all(block, "zero", split_axis=0, concat_axis=0, tiled=True)

    scale = [None] * len(chunks)
    own_max = column_max(*pairs[0], 0, lead)
    scale[0] = jnp.max(lax.all_gather(own_max, "zero"), axis=0)
    thin = [narrow(*pairs[0], scale[0], 0, lead, parts)]
    later, _ = lax.optimization_barrier((pairs, thin[0]))
    rest = [column_max(*later[t], f, c) for t, f, c in chunks[1:]]
    scale[1:] = lax.pmax(rest, "zero")
    got = [exchange(thin[0])]
    for k in range(1, len(chunks)):
        t, f, c = chunks[k]
        thin.append(narrow(*pairs[t], scale[k], f, c, parts))
        if k == 2:
            router_weight, _ = lax.optimization_barrier((router_weight, thin[k]))
            serve_router = route(router_weight, router_gain)
            thin[k], serve_router = lax.optimization_barrier((thin[k], serve_router))
        block, _ = lax.optimization_barrier((thin[k], got[k - 1]))
        got.append(exchange(block))
    ready, own = [], []
    for t in range(2):
        held = None
        for k, (u, f, c) in enumerate(chunks):
            if u == t:
                held = place(got[k], held, f, experts)
        ready.append(jnp.swapaxes(held, 1, 2))
        both = jnp.concatenate([scale[k][:, 0] for k, (u, _, _) in enumerate(chunks) if u == t])
        own.append(lax.dynamic_slice_in_dim(both, lax.axis_index("zero") * width, width, axis=1))
    return (*ready, *own, serve_router)


def solution(mesh):
    parts = mesh.shape["zero"]

    def on_device(train_gate, *others):
        experts, rows, columns = train_gate.shape
        if rows % 128 == 0 and columns % (16 * parts) == 0 and experts % 4 == 0:
            return chunked(parts, train_gate, *others)
        return plain(train_gate, *others)

    return jax.shard_map(
        on_device,
        mesh=mesh,
        in_specs=(
            P("bank", "zero", None),
            P("bank", "zero", None),
            P("bank", "zero", None),
            P("bank", "zero", None),
            P("zero", "bank"),
            P("zero"),
        ),
        out_specs=(
            P("bank", None, "zero"),
            P("bank", None, "zero"),
            P("bank", "zero"),
            P("bank", "zero"),
            P(),
        ),
        check_vma=False,
    )
```
